32 devices in a mesh: blk: 8 (over y, x, core), grp: 4 (over z).
Axes of the slice: x: 2, y: 2, z: 4, core: 2. Of those that a mesh axis runs over, the one named last changes fastest.
Arguments:
- queries: bfloat16 [8192, 4096], P(('blk', 'grp')), may hold values from -1 to 1
- documents: bfloat16 [8192, 4096], P(('blk', 'grp')), may hold values from -1 to 1
- positives: int32 [32, 256], P(('blk', 'grp')), may hold values from 0 to 255, as said below
Outputs:
- query_grad: float32 [8192, 4096], P(('blk', 'grp'))
- doc_grad: float32 [8192, 4096], P(('blk', 'grp'))
- loss: float32 [], replicated
The draws below stay inside these ranges and needn't reach their ends.
Inputs may be any that keep to these rules, and one draw needn't show every extreme that they name: `positives`: each block of 256 rows names each of 0 to 255 exactly once.
All inputs are finite; a program needn't handle non-finite values.
Results may differ from the reference program's by a relative error of at most 0.0036.
Values may be sent and summed in bfloat16 or wider, within the bound.
A program may use at most 128 MiB of HBM per device.

```python
import jax
import jax.numpy as jnp
from jax import lax

D = 4096
ROWS = 256
TOTAL = 8192
N_BLK = 8
N_GRP = 4


def common_draw(key):
    key_noise = jax.random.fold_in(key, 11)
    key_docs = jax.random.fold_in(key, 12)
    key_perm = jax.random.fold_in(key, 13)
    blocks = N_BLK * N_GRP
    perm_keys = jax.random.split(key_perm, blocks)
    positives = jax.vmap(lambda k: jax.random.permutation(k, ROWS))(perm_keys).astype(jnp.int32)
    docs = jax.random.normal(key_docs, (TOTAL, D), jnp.float32) * D ** (-0.5)
    noise = jax.random.normal(key_noise, (TOTAL, D), jnp.float32) * D ** (-0.5)
    span = 0.12
    rows = jnp.arange(TOTAL, dtype=jnp.int32)
    block = rows // ROWS
    shard = (block // N_GRP).astype(jnp.float32)
    align = span * shard / (N_BLK - 1)
    target = block * ROWS + positives.reshape(-1)
    paired = docs[target]
    raw_q = jnp.sqrt(1.0 - align * align)[:, None] * noise + align[:, None] * paired
    return (raw_q, docs, positives)


def draw_queries(key, part):
    return common_draw(key)[0].astype(jnp.bfloat16)


def draw_documents(key, part):
    return common_draw(key)[1].astype(jnp.bfloat16)


def draw_positives(key, part):
    return common_draw(key)[2]


def setup_inputs(seed: int = 0) -> dict:
    keys = jax.random.split(jax.random.key(seed), 4)
    queries = draw_queries(jax.random.fold_in(keys[3], 71), 0)
    documents = draw_documents(jax.random.fold_in(keys[3], 71), 0)
    positives = draw_positives(jax.random.fold_in(keys[3], 71), 0)
    return {"queries": queries, "documents": documents, "positives": positives}


SCALE = 50.0
EPSILON = 1e-06

def normalize(raw):
    wide = raw.astype(jnp.float32)
    ratio = lax.rsqrt(lax.optimization_barrier(jnp.sum(wide * wide, axis=-1, keepdims=True)) + EPSILON)
    return ((wide * ratio).astype(jnp.bfloat16), ratio)

def pull_back(grad, wide, ratio):
    inner = lax.optimization_barrier(jnp.sum(wide * grad, axis=-1, keepdims=True))
    return ratio * grad - ratio * ratio * ratio * inner * wide

def reference(queries, documents, positives):
    far = N_BLK // 4
    offsets = [0, 1, -1, far, -far]
    norm_q, ratio_q = normalize(queries)
    norm_d, ratio_d = normalize(documents)
    eq4 = norm_q.reshape(N_BLK, N_GRP, ROWS, D)
    ed4 = norm_d.reshape(N_BLK, N_GRP, ROWS, D)
    rq4 = ratio_q.reshape(N_BLK, N_GRP, ROWS, 1)
    rd4 = ratio_d.reshape(N_BLK, N_GRP, ROWS, 1)
    raw_q = queries.reshape(N_BLK, N_GRP, ROWS, D)
    raw_d = documents.reshape(N_BLK, N_GRP, ROWS, D)
    pos4 = positives.reshape(N_BLK, N_GRP, ROWS)
    columns = jnp.arange(ROWS, dtype=jnp.int32)

    def hot_of(index):
        return (columns[None, None, :] == pos4[index][:, :, None]).astype(jnp.float32)

    def forward(index):
        cand = jnp.stack([ed4[jnp.mod(index - off, N_BLK).astype(jnp.int32)] for off in offsets]).astype(jnp.float32)
        left = eq4[index].astype(jnp.float32)
        scores = SCALE * jnp.einsum('gid,cgjd->cgij', left, cand)
        lse = jnp.log(lax.optimization_barrier(jnp.sum(jnp.exp(scores), axis=(0, 3))))
        hot = hot_of(index)
        spos = lax.optimization_barrier(jnp.sum(scores[0] * hot, axis=-1))
        part = jnp.sum(lse - spos)
        probs = jnp.exp(scores - lse[None, :, :, None])
        probs = jnp.concatenate([(probs[0] - hot)[None], probs[1:]], axis=0)
        weights = probs.astype(jnp.bfloat16).astype(jnp.float32)
        direction = SCALE * jnp.einsum('cgij,cgjd->gid', weights, cand)
        grad = pull_back(direction, raw_q[index].astype(jnp.float32), rq4[index])
        return (grad, lse, part)
    grads_q, lses, parts = lax.map(forward, jnp.arange(N_BLK, dtype=jnp.int32))

    def backward(index):
        right = ed4[index].astype(jnp.float32)
        total = jnp.zeros((N_GRP, ROWS, D), jnp.float32)
        for off in offsets:
            source = jnp.mod(index + off, N_BLK).astype(jnp.int32)
            left = eq4[source].astype(jnp.float32)
            scores = SCALE * jnp.einsum('gid,gjd->gij', left, right)
            probs = jnp.exp(scores - lses[source][:, :, None])
            if off == 0:
                probs = probs - hot_of(index)
            weights = probs.astype(jnp.bfloat16).astype(jnp.float32)
            total = total + SCALE * jnp.einsum('gij,gid->gjd', weights, left)
        return pull_back(total, raw_d[index].astype(jnp.float32), rd4[index])
    grads_d = lax.map(backward, jnp.arange(N_BLK, dtype=jnp.int32))
    loss = jnp.sum(parts) / TOTAL
    return (grads_q.reshape(TOTAL, D), grads_d.reshape(TOTAL, D), loss)
```

```python
import functools

import jax
import jax.numpy as jnp
from jax import lax
from jax.experimental import pallas as pl
from jax.experimental.pallas import tpu as pltpu
from jax.sharding import PartitionSpec as P

SCALE = 50.0
EPSILON = 1e-06


def from_behind(value, axis, steps):
    count = lax.axis_size(axis)
    pairs = [(source, (source + steps) % count) for source in range(count)]
    return lax.ppermute(value, axis, pairs)


def normalize(raw):
    wide = raw.astype(jnp.float32)
    ratio = lax.rsqrt(jnp.sum(wide * wide, axis=-1, keepdims=True) + EPSILON)
    return ((wide * ratio).astype(jnp.bfloat16), wide, ratio)


def pull_back(grad, wide, ratio):
    inner = jnp.sum(wide * grad, axis=-1, keepdims=True)
    return ratio * grad - ratio * ratio * ratio * inner * wide


def score_block(left, right):
    return SCALE * jnp.einsum("id,jd->ij", left, right, preferred_element_type=jnp.float32)


def transpose_product(weights, left):
    return SCALE * jnp.einsum("ij,id->jd", weights, left, preferred_element_type=jnp.float32)


def on_device_plain(queries, documents, positives):
    norm_q, wide_q, ratio_q = normalize(queries)
    norm_d, wide_d, ratio_d = normalize(documents)
    width = lax.axis_size("blk")
    far = width // 4
    offsets = [1, -1, far, -far]
    rows = norm_q.shape[0]
    received = [norm_d]
    for off in offsets:
        received.append(from_behind(norm_d, "blk", off))
    scores = [score_block(norm_q, block) for block in received]
    total = scores[0].shape[0] * 0.0 + jnp.zeros((rows,), jnp.float32)
    for block_scores in scores:
        total = total + jnp.sum(jnp.exp(block_scores), axis=-1)
    lse = jnp.log(total)
    columns = jnp.arange(rows, dtype=jnp.int32)
    hot = (columns[None, :] == positives[0][:, None]).astype(jnp.float32)
    spos = jnp.sum(scores[0] * hot, axis=-1)
    part = jnp.sum(lse - spos)
    weights = [(jnp.exp(scores[0] - lse[:, None]) - hot).astype(jnp.bfloat16)]
    for block_scores in scores[1:]:
        weights.append(jnp.exp(block_scores - lse[:, None]).astype(jnp.bfloat16))
    query_dir = jnp.zeros_like(wide_q)
    for weight, block in zip(weights, received):
        query_dir = query_dir + SCALE * jnp.dot(weight, block, preferred_element_type=jnp.float32)
    doc_dir = transpose_product(weights[0], norm_q)
    for off, weight in zip(offsets, weights[1:]):
        partial_grad = transpose_product(weight, norm_q)
        doc_dir = doc_dir + from_behind(partial_grad.astype(jnp.bfloat16), "blk", -off).astype(
            partial_grad.dtype
        )
    query_grad = pull_back(query_dir, wide_q, ratio_q)
    doc_grad = pull_back(doc_dir, wide_d, ratio_d)
    summed = lax.psum(part, ("blk", "grp"))
    loss = summed / (rows * width * lax.axis_size("grp"))
    return (query_grad, doc_grad, loss)

CORES = 2
MESH = pl.DeviceIdType.MESH
CHUNK = 32
AHEAD = 3
TILE = 512
DEEP = 1024
NEAR, DIAG, RELAY, SIBLING = range(4)


def columns(n, size):
    return pl.ds(pl.multiple_of(n * size, size), size)


def wide_dot(left, right, contract):
    return lax.dot_general(left, right, ((contract[:1], contract[1:]), ((), ())), preferred_element_type=jnp.float32)


def kernel(
    n_blk, n_grp,
    queries, documents, positives,
    query_grad, doc_grad, loss,
    own, got, norm_d, norm_q, group_q, scores, weights, turned, ratio_q, ratio_d, inner,
    lse_own, lse_got, lse_wide, sums, sums_got,
    load_sem, x_send, x_recv, y_send, y_recv, r_send, r_recv, s_send, s_recv, l_send, l_recv, t_send, t_recv,
):
    rows, width = queries.shape
    per = rows // CHUNK
    chunks = 2 * per
    me, grp = lax.axis_index("blk"), lax.axis_index("grp")
    core, x, y = me % 2, (me // 2) % 2, me // 4
    sibling = me + 1 - 2 * core
    near = me + 2 - 4 * x
    across = me + 4 - 8 * y
    diag = near + 4 - 8 * y
    relay = lax.rem(me + n_blk - 1 + 2 * core, n_blk)
    relay_from = lax.rem(x + core, 2)
    grp_bits = [1 << n for n in range(n_grp.bit_length() - 1)]
    peers = [(sibling, grp), (near, grp), (across, grp)]
    for bit in grp_bits:
        peers.append((me, grp + bit - 2 * bit * ((grp // bit) % 2)))

    def remote(source, target, send, recv, device):
        return pltpu.make_async_remote_copy(
            src_ref=source, dst_ref=target, send_sem=send, recv_sem=recv, device_id=device, device_id_type=MESH
        )

    def piece(n):
        return pl.ds(pl.multiple_of(n * CHUNK, CHUNK), CHUNK)

    def x_copy(n):
        return remote(own.at[piece(n)], got.at[NEAR, piece(n)], x_send.at[n], x_recv.at[n], (near, grp))

    def y_copy(n):
        return remote(got.at[NEAR, piece(n)], got.at[DIAG, piece(n)], y_send.at[n], y_recv.at[n], (across, grp))

    def r_copy(n):
        return remote(
            got.at[relay_from, piece(n)], got.at[RELAY, piece(n)], r_send.at[n], r_recv.at[n], (sibling, grp)
        )

    def s_copy(half):
        cut = pl.ds(half * rows, rows)
        return remote(own.at[cut], got.at[SIBLING, cut], s_send.at[half], s_recv.at[half], (sibling, grp))

    lse_peers = [near, diag, relay, sibling]

    def lse_copy(n):
        return remote(lse_own, lse_got.at[n], l_send.at[n], l_recv.at[n], (lse_peers[n], grp))

    def sum_copy(n):
        return remote(sums.at[n], sums_got.at[n], t_send.at[n], t_recv.at[n], peers[n])

    load_d = pltpu.make_async_copy(documents, own.at[pl.ds(0, rows)], load_sem.at[0])
    load_q = pltpu.make_async_copy(queries, own.at[pl.ds(rows, rows)], load_sem.at[1])
    load_d.start()
    load_q.start()
    barrier = pltpu.get_barrier_semaphore()
    greeted = peers + [(diag, grp), (relay, grp)]
    for device in greeted:
        pl.semaphore_signal(barrier, inc=1, device_id=device, device_id_type=MESH)
    pl.semaphore_wait(barrier, len(greeted))
    load_d.wait()
    for n in range(AHEAD):
        x_copy(n).start()
    s_copy(0).start()
    load_q.wait()

    def normalized(raw):
        wide = raw.astype(jnp.float32)
        ratio = lax.rsqrt(jnp.sum(wide * wide, axis=-1, keepdims=True) + EPSILON)
        return (wide * ratio).astype(jnp.bfloat16), ratio

    def normalize_own(n, _):
        cut = piece(n)
        norm_d[cut, :], ratio_d[cut, :] = normalized(own[cut, :])
        norm_q[cut, :], ratio_q[cut, :] = normalized(own[piece(n + per), :])
        return 0

    def score(left, right, right_rows, target):
        def body(n, _):
            cut = columns(n, DEEP)
            term = SCALE * wide_dot(left[:, cut], right[right_rows, cut], (1, 1))

            @pl.when(n == 0)
            def _():
                target[...] = term

            @pl.when(n > 0)
            def _():
                target[...] += term
            return 0

        lax.fori_loop(0, width // DEEP, body, 0)

    def transposed(value):
        return jnp.transpose(value)

    def add_doc_terms(left, first):
        def body(n, _):
            cut = columns(n, TILE)
            term = SCALE * wide_dot(turned[...], left[:, cut], (1, 0))
            doc_grad[:, cut] = term if first else doc_grad[:, cut] + term
            return 0

        lax.fori_loop(0, width // TILE, body, 0)

    def pull_back_into(grad, raw_rows, ratio_ref):
        inner[...] = jnp.zeros_like(inner)

        def gather(n, _):
            cut = columns(n, TILE)
            prod = own[raw_rows, cut].astype(jnp.float32) * grad[:, cut]
            total = prod[:, :128]
            for k in range(1, TILE // 128):
                total = total + prod[:, k * 128 : (k + 1) * 128]
            inner[...] += total
            return 0

        lax.fori_loop(0, width // TILE, gather, 0)
        ratio = ratio_ref[...]
        factor = ratio * ratio * ratio * jnp.sum(inner[...], axis=-1, keepdims=True)

        def spread(n, _):
            cut = columns(n, TILE)
            grad[:, cut] = ratio * grad[:, cut] - factor * own[raw_rows, cut].astype(jnp.float32)
            return 0

        lax.fori_loop(0, width // TILE, spread, 0)

    def pump(n):
        if n < chunks:
            x_copy(n).wait_recv()
            y_copy(n).start()
            if n + AHEAD < chunks:
                x_copy(n + AHEAD).start()
        if 0 <= n - 2 < chunks:
            y_copy(n - 2).wait_recv()
            r_copy(n - 2).start()
        if 0 <= n - 3 < chunks:
            r_copy(n - 3).wait_recv()

    def normalize_documents(n):
        for k in (NEAR, DIAG, RELAY):
            norm_d[pl.ds((2 + k) * rows + n * CHUNK, CHUNK), :] = normalized(got[k, pl.ds(n * CHUNK, CHUNK), :])[0]

    def normalize_group(n):
        step = rows // 4
        for k in (NEAR, DIAG, RELAY, SIBLING):
            def body(m, _, k=k):
                value = got[k, pl.ds(pl.multiple_of(rows + n * step + m * 16, 16), 16), :]
                group_q[pl.ds(pl.multiple_of(k * step + m * 16, 16), 16), :] = normalized(value)[0]
                return 0
            lax.fori_loop(0, step // 16, body, 0)

    def add_group(n):
        step = rows // 4
        score(group_q, norm_d, pl.ds(0, rows), scores.at[:, pl.ds(0, rows)])
        lse = jnp.concatenate([lse_wide[k, n * step : (n + 1) * step, :] for k in range(4)], axis=0)[:, :1]
        turned[...] = transposed(jnp.exp(scores[:, :rows] - lse)).astype(jnp.bfloat16)
        add_doc_terms(group_q, False)

    lax.fori_loop(0, per, normalize_own, 0)
    s_copy(1).start()
    score(norm_q, norm_d, pl.ds(0, rows), scores.at[:, pl.ds(0, rows)])
    pump(0)
    s_copy(0).wait_recv()

    def normalize_sibling(n, _):
        cut = pl.ds(pl.multiple_of(rows + n * CHUNK, CHUNK), CHUNK)
        norm_d[cut, :] = normalized(got[SIBLING, piece(n), :])[0]
        return 0

    lax.fori_loop(0, per, normalize_sibling, 0)
    score(norm_q, norm_d, pl.ds(rows, rows), scores.at[:, pl.ds(rows, rows)])
    for n in range(1, per + 3):
        pump(n)
        if n >= 3:
            normalize_documents(n - 3)
    score(norm_q, norm_d, pl.ds(2 * rows, 3 * rows), scores.at[:, pl.ds(2 * rows, 3 * rows)])
    total = jnp.zeros((rows, 1), jnp.float32)
    for k in range(5):
        total = total + jnp.sum(jnp.exp(scores[:, k * rows : (k + 1) * rows]), axis=-1, keepdims=True)
    lse = jnp.log(total)
    lse_own[...] = transposed(jnp.broadcast_to(lse, (rows, 128)))[:8, :]
    named = jnp.broadcast_to(positives[...].astype(jnp.float32), (rows, rows))
    place = lax.broadcasted_iota(jnp.int32, (rows, rows), 0).astype(jnp.float32)
    hot = transposed((place == named).astype(jnp.float32))
    for k in range(5):
        value = jnp.exp(scores[:, k * rows : (k + 1) * rows] - lse)
        if k == 0:
            value = value - hot
            turned[...] = transposed(value).astype(jnp.bfloat16)
        weights[:, k * rows : (k + 1) * rows] = value.astype(jnp.bfloat16)
    part = jnp.sum(lse) - jnp.sum(scores[:, :rows] * hot)
    sums[0] = jnp.full((8, 128), part, jnp.float32)
    pump(per + 3)
    for k in range(4):
        lse_copy(k).start()
    sum_copy(0).start()

    def query_terms(n, _):
        cut = columns(n, TILE)
        query_grad[:, cut] = SCALE * wide_dot(weights[...], norm_d[:, cut], (1, 0))
        return 0

    lax.fori_loop(0, width // TILE, query_terms, 0)
    pump(per + 4)
    pull_back_into(query_grad, pl.ds(rows, rows), ratio_q)
    add_doc_terms(norm_q, True)
    s_copy(1).wait_recv()
    for k in range(4):
        lse_copy(k).wait_recv()
        value = jnp.broadcast_to(lse_got[k, :1, :], (128, rows))
        lse_wide[k] = transposed(value)
    done = 0
    rounds = 0

    def next_round(rounds):
        sum_copy(rounds).wait_recv()
        sums[rounds + 1] = sums[rounds] + sums_got[rounds]

    for n in range(per + 5, chunks + 3):
        pump(n)
        if rounds < len(peers):
            next_round(rounds)
            rounds += 1
        ready = (n - 3 - per + 1) * 4 // per
        while done < ready:
            normalize_group(done)
            add_group(done)
            done += 1
        if 0 < rounds < len(peers):
            sum_copy(rounds).start()
    while rounds < len(peers):
        next_round(rounds)
        rounds += 1
        if rounds < len(peers):
            sum_copy(rounds).start()
    pull_back_into(doc_grad, pl.ds(0, rows), ratio_d)
    loss[0, 0] = jnp.max(sums[len(peers)]) / (rows * n_blk * n_grp)

    def drain(n, _):
        x_copy(n).wait_send()
        y_copy(n).wait_send()
        r_copy(n).wait_send()
        return 0

    lax.fori_loop(0, chunks, drain, 0)
    for half in range(2):
        s_copy(half).wait_send()
    for k in range(4):
        lse_copy(k).wait_send()
    for k in range(len(peers)):
        sum_copy(k).wait_send()


def on_device_relay(queries, documents, positives):
    n_blk, n_grp = lax.axis_size("blk"), lax.axis_size("grp")
    rows, width = queries.shape
    chunks = 2 * rows // CHUNK
    rounds = 3 + n_grp.bit_length() - 1
    narrow, wide = jnp.bfloat16, jnp.float32
    dma = pltpu.SemaphoreType.DMA
    grad = pltpu.VMEM((rows, width), wide)
    query_grad, doc_grad, loss = pl.pallas_call(
        functools.partial(kernel, n_blk, n_grp),
        out_shape=[grad, grad, jax.ShapeDtypeStruct((1, 1), wide)],
        in_specs=[
            pl.BlockSpec(memory_space=pl.ANY),
            pl.BlockSpec(memory_space=pl.ANY),
            pl.BlockSpec(memory_space=pltpu.VMEM),
        ],
        out_specs=[
            pl.BlockSpec(memory_space=pltpu.VMEM),
            pl.BlockSpec(memory_space=pltpu.VMEM),
            pl.BlockSpec(memory_space=pltpu.SMEM),
        ],
        scratch_shapes=[
            pltpu.VMEM((2 * rows, width), narrow),
            pltpu.VMEM((4, 2 * rows, width), narrow),
            pltpu.VMEM((5 * rows, width), narrow),
            pltpu.VMEM((rows, width), narrow),
            pltpu.VMEM((rows, width), narrow),
            pltpu.VMEM((rows, 5 * rows), wide),
            pltpu.VMEM((rows, 5 * rows), narrow),
            pltpu.VMEM((rows, rows), narrow),
            pltpu.VMEM((rows, 1), wide),
            pltpu.VMEM((rows, 1), wide),
            pltpu.VMEM((rows, 128), wide),
            pltpu.VMEM((8, rows), wide),
            pltpu.VMEM((4, 8, rows), wide),
            pltpu.VMEM((4, rows, 128), wide),
            pltpu.VMEM((rounds + 1, 8, 128), wide),
            pltpu.VMEM((rounds, 8, 128), wide),
            dma((2,)),
            dma((chunks,)), dma((chunks,)), dma((chunks,)), dma((chunks,)), dma((chunks,)), dma((chunks,)),
            dma((2,)), dma((2,)), dma((4,)), dma((4,)), dma((rounds,)), dma((rounds,)),
        ],
        compiler_params=pltpu.CompilerParams(
            collective_id=0, has_side_effects=True, vmem_limit_bytes=52 * 1024 * 1024
        ),
    )(queries, documents, positives)
    return query_grad, doc_grad, loss.reshape(())


def fits(n_blk, n_grp):
    return n_blk == 4 * CORES and n_grp & (n_grp - 1) == 0


def on_device(queries, documents, positives):
    if fits(lax.axis_size("blk"), lax.axis_size("grp")):
        return on_device_relay(queries, documents, positives)
    return on_device_plain(queries, documents, positives)


def solution(mesh):
    return jax.shard_map(
        on_device,
        mesh=mesh,
        in_specs=(P(("blk", "grp"), None), P(("blk", "grp"), None), P(("blk", "grp"), None)),
        out_specs=(P(("blk", "grp"), None), P(("blk", "grp"), None), P()),
        check_vma=False,
    )
```

```python
import functools

import jax
import jax.numpy as jnp
from jax import lax
from jax.experimental import pallas as pl
from jax.experimental.pallas import tpu as pltpu
from jax.sharding import PartitionSpec as P

SCALE = 50.0
EPSILON = 1e-06


def from_behind(value, axis, steps):
    count = lax.axis_size(axis)
    pairs = [(source, (source + steps) % count) for source in range(count)]
    return lax.ppermute(value, axis, pairs)


def normalize(raw):
    wide = raw.astype(jnp.float32)
    ratio = lax.rsqrt(jnp.sum(wide * wide, axis=-1, keepdims=True) + EPSILON)
    return ((wide * ratio).astype(jnp.bfloat16), wide, ratio)


def pull_back(grad, wide, ratio):
    inner = jnp.sum(wide * grad, axis=-1, keepdims=True)
    return ratio * grad - ratio * ratio * ratio * inner * wide


def score_block(left, right):
    return SCALE * jnp.einsum("id,jd->ij", left, right, preferred_element_type=jnp.float32)


def transpose_product(weights, left):
    return SCALE * jnp.einsum("ij,id->jd", weights, left, preferred_element_type=jnp.float32)


def on_device_plain(queries, documents, positives):
    norm_q, wide_q, ratio_q = normalize(queries)
    norm_d, wide_d, ratio_d = normalize(documents)
    width = lax.axis_size("blk")
    far = width // 4
    offsets = [1, -1, far, -far]
    rows = norm_q.shape[0]
    received = [norm_d]
    for off in offsets:
        received.append(from_behind(norm_d, "blk", off))
    scores = [score_block(norm_q, block) for block in received]
    total = scores[0].shape[0] * 0.0 + jnp.zeros((rows,), jnp.float32)
    for block_scores in scores:
        total = total + jnp.sum(jnp.exp(block_scores), axis=-1)
    lse = jnp.log(total)
    columns = jnp.arange(rows, dtype=jnp.int32)
    hot = (columns[None, :] == positives[0][:, None]).astype(jnp.float32)
    spos = jnp.sum(scores[0] * hot, axis=-1)
    part = jnp.sum(lse - spos)
    weights = [(jnp.exp(scores[0] - lse[:, None]) - hot).astype(jnp.bfloat16)]
    for block_scores in scores[1:]:
        weights.append(jnp.exp(block_scores - lse[:, None]).astype(jnp.bfloat16))
    query_dir = jnp.zeros_like(wide_q)
    for weight, block in zip(weights, received):
        query_dir = query_dir + SCALE * jnp.dot(weight, block, preferred_element_type=jnp.float32)
    doc_dir = transpose_product(weights[0], norm_q)
    for off, weight in zip(offsets, weights[1:]):
        partial_grad = transpose_product(weight, norm_q)
        doc_dir = doc_dir + from_behind(partial_grad.astype(jnp.bfloat16), "blk", -off).astype(
            partial_grad.dtype
        )
    query_grad = pull_back(query_dir, wide_q, ratio_q)
    doc_grad = pull_back(doc_dir, wide_d, ratio_d)
    summed = lax.psum(part, ("blk", "grp"))
    loss = summed / (rows * width * lax.axis_size("grp"))
    return (query_grad, doc_grad, loss)

CORES = 2
MESH = pl.DeviceIdType.MESH
CHUNK = 16
SPLIT = 1
PARTS = 8
LAG = 2
BUDGET = 3.5
GROUPS = (10, 4, 2)
AHEAD = 2
TILE = 512
DEEP = 1024
NEAR, DIAG, RELAY, SIBLING = range(4)


def columns(n, size):
    return pl.ds(pl.multiple_of(n * size, size), size)


def wide_dot(left, right, contract):
    return lax.dot_general(left, right, ((contract[:1], contract[1:]), ((), ())), preferred_element_type=jnp.float32)


def kernel(
    n_blk, n_grp,
    queries, documents, positives,
    query_grad, doc_grad, loss,
    own, got, norm_d, norm_q, sibling_q, group_q, scores, group_scores, weights, turned, ratio_q, ratio_d, inner,
    lse_own, lse_got, lse_wide, lse_group, sums, sums_got,
    load_sem, x_send, x_recv, y_send, y_recv, r_send, r_recv, s_send, s_recv, l_send, l_recv, t_send, t_recv,
):
    rows, width = queries.shape
    per = rows // CHUNK
    copies = 2 * per * SPLIT
    part_rows = 2 * rows // PARTS
    me, grp = lax.axis_index("blk"), lax.axis_index("grp")
    core, x, y = me % 2, (me // 2) % 2, me // 4
    sibling = me + 1 - 2 * core
    near = me + 2 - 4 * x
    across = me + 4 - 8 * y
    diag = near + 4 - 8 * y
    relay = lax.rem(me + n_blk - 1 + 2 * core, n_blk)
    relay_from = lax.rem(x + core, 2)
    peers = [(sibling, grp), (near, grp), (across, grp)]
    for bit in [1 << n for n in range(n_grp.bit_length() - 1)]:
        peers.append((me, grp + bit - 2 * bit * ((grp // bit) % 2)))

    def remote(source, target, send, recv, device):
        return pltpu.make_async_remote_copy(
            src_ref=source, dst_ref=target, send_sem=send, recv_sem=recv, device_id=device, device_id_type=MESH
        )

    def piece(n):
        size = width // SPLIT
        return (
            pl.ds(pl.multiple_of((n // SPLIT) * CHUNK, CHUNK), CHUNK),
            pl.ds(pl.multiple_of((n % SPLIT) * size, size), size),
        )

    def x_copy(n):
        r, c = piece(n)
        return remote(own.at[r, c], got.at[NEAR, r, c], x_send.at[n], x_recv.at[n], (near, grp))

    def y_copy(n):
        r, c = piece(n)
        return remote(got.at[NEAR, r, c], got.at[DIAG, r, c], y_send.at[n], y_recv.at[n], (across, grp))

    def r_copy(n):
        r, c = piece(n)
        return remote(got.at[relay_from, r, c], got.at[RELAY, r, c], r_send.at[n], r_recv.at[n], (sibling, grp))

    def s_copy(n):
        cut = pl.ds(n * part_rows, part_rows)
        return remote(own.at[cut], got.at[SIBLING, cut], s_send.at[n], s_recv.at[n], (sibling, grp))

    lse_peers = [near, diag, relay, sibling]

    def lse_copy(n):
        return remote(lse_own, lse_got.at[n], l_send.at[n], l_recv.at[n], (lse_peers[n], grp))

    def sum_copy(n):
        return remote(sums.at[n], sums_got.at[n], t_send.at[n], t_recv.at[n], peers[n])

    load_d = pltpu.make_async_copy(documents, own.at[pl.ds(0, rows)], load_sem.at[0])
    load_q = pltpu.make_async_copy(queries, own.at[pl.ds(rows, rows)], load_sem.at[1])
    load_d.start()
    load_q.start()
    group_scores[...] = jnp.zeros_like(group_scores)
    barrier = pltpu.get_barrier_semaphore()
    greeted = peers + [(diag, grp), (relay, grp)]
    for device in greeted:
        pl.semaphore_signal(barrier, inc=1, device_id=device, device_id_type=MESH)
    pl.semaphore_wait(barrier, len(greeted))
    load_d.wait()
    for n in range(AHEAD):
        x_copy(n).start()
    load_q.wait()

    def normalized(raw):
        wide = raw.astype(jnp.float32)
        ratio = lax.rsqrt(jnp.sum(wide * wide, axis=-1, keepdims=True) + EPSILON)
        return (wide * ratio).astype(jnp.bfloat16), ratio

    def at(start, size):
        return pl.ds(start, size)

    def normalize_own(first):
        for start in range(first, first + 32, 16):
            cut = at(start, 16)
            norm_d[cut, :], ratio_d[cut, :] = normalized(own[cut, :])
            norm_q[cut, :], ratio_q[cut, :] = normalized(own[at(rows + start, 16), :])

    def normalize_into(target, target_row, source, row, count):
        for start in range(0, count, 16):
            target[at(target_row + start, 16), :] = normalized(got[source, at(row + start, 16), :])[0]

    def score(left, left_rows, right, right_rows, target):
        def body(n, _):
            cut = columns(n, DEEP)
            term = SCALE * wide_dot(left[left_rows, cut], right[right_rows, cut], (1, 1))

            @pl.when(n == 0)
            def _():
                target[...] = term

            @pl.when(n > 0)
            def _():
                target[...] += term
            return 0

        lax.fori_loop(0, width // DEEP, body, 0)

    def loop(first, last, body):
        lax.fori_loop(first, last, lambda n, _: (body(n), 0)[1], 0)

    tiles = width // TILE

    def doc_terms(left, left_rows, depth, place, first, low, high):
        def body(n):
            cut = columns(n, TILE)
            term = SCALE * wide_dot(turned[:, place : place + depth], left[left_rows, cut], (1, 0))
            doc_grad[:, cut] = term if first else doc_grad[:, cut] + term

        loop(low, high, body)

    def gather(grad, raw_rows):
        inner[...] = jnp.zeros_like(inner)

        def body(n):
            cut = columns(n, TILE)
            prod = own[raw_rows, cut].astype(jnp.float32) * grad[:, cut]
            total = prod[:, :128]
            for k in range(1, TILE // 128):
                total = total + prod[:, k * 128 : (k + 1) * 128]
            inner[...] += total

        loop(0, tiles, body)

    def spread(grad, raw_rows, ratio_ref):
        ratio = ratio_ref[...]
        factor = ratio * ratio * ratio * jnp.sum(inner[...], axis=-1, keepdims=True)

        def body(n):
            cut = columns(n, TILE)
            grad[:, cut] = ratio * grad[:, cut] - factor * own[raw_rows, cut].astype(jnp.float32)

        loop(0, tiles, body)

    soon, later, state = [], [], {"now": 0, "lse": False}
    all_rows = at(0, rows)
    doc_rows, query_rows = at(0, rows), at(rows, rows)

    def block(k):
        return pl.ds(k * rows, rows)

    def put(ready, cost, step):
        later.append((ready, cost, step))

    def in_(delay, step):
        soon.append((state["now"] + delay, step))

    def send_sibling(n):
        s_copy(n).start()

    for n in range(PARTS):
        soon.append((n * SPLIT, functools.partial(send_sibling, n)))
    for first in range(0, rows, 32):
        put(0, 0.3, functools.partial(normalize_own, first))
    put(0, 1.2, lambda: score(norm_q, all_rows, norm_d, block(0), scores.at[:, block(0)]))

    def sibling_part(n):
        s_copy(n).wait_recv()
        row = n * part_rows
        if row < rows:
            normalize_into(norm_d, rows + row, SIBLING, row, part_rows)
        else:
            normalize_into(sibling_q, row - rows, SIBLING, row, part_rows)

    for n in range(PARTS):
        put((n + 2) * SPLIT, 0.3 * part_rows / 64, functools.partial(sibling_part, n))
        if (n + 1) * 2 == PARTS:
            put(0, 1.2, lambda: score(norm_q, all_rows, norm_d, block(1), scores.at[:, block(1)]))
    put(0, 1.2, lambda: score(sibling_q, all_rows, norm_d, block(0), scores.at[:, block(5)]))

    def arrived(n):
        if n < per:
            for k in (NEAR, DIAG, RELAY):
                normalize_into(norm_d, (2 + k) * rows + n * CHUNK, k, n * CHUNK, CHUNK)
        else:
            for k in (NEAR, DIAG, RELAY):
                normalize_into(group_q, ((n - per) * 3 + k) * CHUNK, k, n * CHUNK, CHUNK)

    for k in (2, 3, 4):
        put(per * SPLIT + 2, 1.2, functools.partial(
            lambda k: score(norm_q, all_rows, norm_d, block(k), scores.at[:, block(k)]), k))

    def log_sum():
        total = jnp.zeros((rows, 1), jnp.float32)
        for k in range(5):
            total = total + jnp.sum(jnp.exp(scores[:, k * rows : (k + 1) * rows]), axis=-1, keepdims=True)
        lse_wide[3] = jnp.broadcast_to(jnp.log(total), (rows, 128))
        lse_own[...] = jnp.transpose(lse_wide[3])[:8, :]
        in_(1, send_lse)

    def send_lse():
        for k in range(4):
            lse_copy(k).start()
        in_(2 * SPLIT, take_lse)

    def take_lse():
        for k in range(4):
            lse_copy(k).wait_recv()
            value = jnp.transpose(jnp.broadcast_to(lse_got[k, :1, :], (128, rows)))
            if k == SIBLING:
                lse_group[pl.ds(0, rows), :] = value
                continue
            for n in range(per):
                lse_group[pl.ds(rows + (n * 3 + k) * CHUNK, CHUNK), :] = value[n * CHUNK : (n + 1) * CHUNK, :]
        state["lse"] = True
        urgent.append((0, 0.3, sibling_weights))
        add_doc_steps(norm_q, all_rows, rows, 0, True)
        add_doc_steps(sibling_q, all_rows, rows, rows, False)

    def add_doc_steps(left, left_rows, depth, place, first, where=None):
        steps = 2 if SPLIT == 1 else 4
        for n in range(steps):
            urgent.append((0, 2.0 / steps, functools.partial(
                doc_terms, left, left_rows, depth, place, first, n * tiles // steps, (n + 1) * tiles // steps)))

    def sibling_weights():
        value = jnp.exp(scores[:, 5 * rows :] - lse_group[pl.ds(0, rows), :][:, :1])
        turned[:, rows : 2 * rows] = jnp.transpose(value).astype(jnp.bfloat16)

    def weight(k):
        value = jnp.exp(scores[:, k * rows : (k + 1) * rows] - lse_wide[3][:, :1])
        if k == 0:
            named = jnp.broadcast_to(positives[...].astype(jnp.float32), (rows, rows))
            place = lax.broadcasted_iota(jnp.int32, (rows, rows), 0).astype(jnp.float32)
            hot = jnp.transpose((place == named).astype(jnp.float32))
            value = value - hot
            turned[:, :rows] = jnp.transpose(value).astype(jnp.bfloat16)
            part = jnp.sum(lse_wide[3][:, :1]) - jnp.sum(scores[:, :rows] * hot)
            sums[0] = jnp.full((8, 128), part, jnp.float32)
            in_(1, functools.partial(send_sum, 0))
        weights[:, k * rows : (k + 1) * rows] = value.astype(jnp.bfloat16)

    def send_sum(n):
        sum_copy(n).start()
        in_(SPLIT, functools.partial(take_sum, n))

    def take_sum(n):
        sum_copy(n).wait_recv()
        sums[n + 1] = sums[n] + sums_got[n]
        if n + 1 < len(peers):
            in_(1, functools.partial(send_sum, n + 1))
        else:
            in_(1, give_loss)

    def give_loss():
        loss[0, 0] = jnp.max(sums[len(peers)]) / (rows * n_blk * n_grp)

    put(0, 1.0, log_sum)
    for k in range(5):
        put(0, 0.4 if k else 0.7, functools.partial(weight, k))

    def query_terms(low, high):
        def body(n):
            cut = columns(n, TILE)
            query_grad[:, cut] = SCALE * wide_dot(weights[...], norm_d[:, cut], (1, 0))

        loop(low, high, body)

    for n in range(0, tiles, 2):
        put(0, 1.0, functools.partial(query_terms, n, n + 2))
    put(0, 0.9, lambda: gather(query_grad, query_rows))
    put(0, 0.9, lambda: spread(query_grad, query_rows, ratio_q))
    urgent = []
    groups, start = [], 0
    for count in GROUPS:
        groups.append((start, count * per // 16))
        start += count * per // 16

    def group(index):
        start, count = groups[index]
        first, depth = start * 3 * CHUNK, count * 3 * CHUNK
        for low in range(0, depth, rows):
            size = min(rows, depth - low)
            urgent.append((0, 1.2, functools.partial(
                score, group_q, at(first + low, size), norm_d, block(0), group_scores.at[at(low, size), :])))

        def group_weights():
            value = jnp.exp(group_scores[at(0, depth), :] - lse_group[pl.ds(rows + first, depth), :][:, :1])
            group_scores[at(0, depth), :] = value
            turned[...] = jnp.transpose(group_scores[...]).astype(jnp.bfloat16)

        urgent.append((0, 0.5, group_weights))
        add_doc_steps(group_q, at(first, depth), depth, 0, False)

    waiting = [(per + start + count - 1, n) for n, (start, count) in enumerate(groups)]
    for n in range(copies + LAG + 1):
        state["now"] = n
        if n < copies:
            x_copy(n).wait_recv()
            y_copy(n).start()
            if n + AHEAD < copies:
                x_copy(n + AHEAD).start()
        m = n - LAG
        if 0 <= m < copies:
            y_copy(m).wait_recv()
            r_copy(m).start()
        m -= 1
        if 0 <= m < copies:
            r_copy(m).wait_recv()
        ready = [step for when, step in soon if when <= n]
        soon[:] = [(when, step) for when, step in soon if when > n]
        for step in ready:
            step()
        if m >= 0 and m % SPLIT == SPLIT - 1 and m < copies:
            arrived(m // SPLIT)
        while waiting and state["lse"] and waiting[0][0] * SPLIT + SPLIT - 1 <= m:
            group(waiting.pop(0)[1])
        spent = 0.0
        while urgent or (later and later[0][0] <= n):
            pool = urgent if urgent else later
            if spent and spent + pool[0][1] > BUDGET / SPLIT:
                break
            ready, cost, step = pool.pop(0)
            step()
            spent += cost
    while soon or urgent or later or waiting:
        state["now"] += 1
        while soon:
            soon.pop(0)[1]()
        while urgent:
            urgent.pop(0)[2]()
        if later:
            later.pop(0)[2]()
        elif waiting and state["lse"]:
            group(waiting.pop(0)[1])
    gather(doc_grad, doc_rows)
    spread(doc_grad, doc_rows, ratio_d)

    def drain(n, _):
        x_copy(n).wait_send()
        y_copy(n).wait_send()
        r_copy(n).wait_send()
        return 0

    lax.fori_loop(0, copies, drain, 0)
    for n in range(PARTS):
        s_copy(n).wait_send()
    for k in range(4):
        lse_copy(k).wait_send()
    for k in range(len(peers)):
        sum_copy(k).wait_send()


def on_device_relay(queries, documents, positives):
    n_blk, n_grp = lax.axis_size("blk"), lax.axis_size("grp")
    rows, width = queries.shape
    copies = 2 * rows // CHUNK * SPLIT
    rounds = 3 + n_grp.bit_length() - 1
    narrow, wide = jnp.bfloat16, jnp.float32
    dma = pltpu.SemaphoreType.DMA
    grad = pltpu.VMEM((rows, width), wide)
    query_grad, doc_grad, loss = pl.pallas_call(
        functools.partial(kernel, n_blk, n_grp),
        out_shape=[grad, grad, jax.ShapeDtypeStruct((1, 1), wide)],
        in_specs=[
            pl.BlockSpec(memory_space=pl.ANY),
            pl.BlockSpec(memory_space=pl.ANY),
            pl.BlockSpec(memory_space=pltpu.VMEM),
        ],
        out_specs=[
            pl.BlockSpec(memory_space=pltpu.VMEM),
            pl.BlockSpec(memory_space=pltpu.VMEM),
            pl.BlockSpec(memory_space=pltpu.SMEM),
        ],
        scratch_shapes=[
            pltpu.VMEM((2 * rows, width), narrow),
            pltpu.VMEM((4, 2 * rows, width), narrow),
            pltpu.VMEM((5 * rows, width), narrow),
            pltpu.VMEM((rows, width), narrow),
            pltpu.VMEM((rows, width), narrow),
            pltpu.VMEM((3 * rows, width), narrow),
            pltpu.VMEM((rows, 6 * rows), wide),
            pltpu.VMEM((2 * rows, rows), wide),
            pltpu.VMEM((rows, 5 * rows), narrow),
            pltpu.VMEM((rows, 2 * rows), narrow),
            pltpu.VMEM((rows, 1), wide),
            pltpu.VMEM((rows, 1), wide),
            pltpu.VMEM((rows, 128), wide),
            pltpu.VMEM((8, rows), wide),
            pltpu.VMEM((4, 8, rows), wide),
            pltpu.VMEM((4, rows, 128), wide),
            pltpu.VMEM((4 * rows, 128), wide),
            pltpu.VMEM((rounds + 1, 8, 128), wide),
            pltpu.VMEM((rounds, 8, 128), wide),
            dma((2,)),
            dma((copies,)), dma((copies,)), dma((copies,)), dma((copies,)), dma((copies,)), dma((copies,)),
            dma((PARTS,)), dma((PARTS,)), dma((4,)), dma((4,)), dma((rounds,)), dma((rounds,)),
        ],
        compiler_params=pltpu.CompilerParams(
            collective_id=0, has_side_effects=True, vmem_limit_bytes=55 * 1024 * 1024
        ),
    )(queries, documents, positives)
    return query_grad, doc_grad, loss.reshape(())


def fits(n_blk, n_grp):
    return n_blk == 4 * CORES and n_grp & (n_grp - 1) == 0


def on_device(queries, documents, positives):
    if fits(lax.axis_size("blk"), lax.axis_size("grp")):
        return on_device_relay(queries, documents, positives)
    return on_device_plain(queries, documents, positives)


def solution(mesh):
    return jax.shard_map(
        on_device,
        mesh=mesh,
        in_specs=(P(("blk", "grp"), None), P(("blk", "grp"), None), P(("blk", "grp"), None)),
        out_specs=(P(("blk", "grp"), None), P(("blk", "grp"), None), P()),
        check_vma=False,
    )
```

```python
import functools

import jax
import jax.numpy as jnp
from jax import lax
from jax.experimental import pallas as pl
from jax.experimental.pallas import tpu as pltpu
from jax.sharding import PartitionSpec as P

SCALE = 50.0
EPSILON = 1e-06


def from_behind(value, axis, steps):
    count = lax.axis_size(axis)
    pairs = [(source, (source + steps) % count) for source in range(count)]
    return lax.ppermute(value, axis, pairs)


def normalize(raw):
    wide = raw.astype(jnp.float32)
    ratio = lax.rsqrt(jnp.sum(wide * wide, axis=-1, keepdims=True) + EPSILON)
    return ((wide * ratio).astype(jnp.bfloat16), wide, ratio)


def pull_back(grad, wide, ratio):
    inner = jnp.sum(wide * grad, axis=-1, keepdims=True)
    return ratio * grad - ratio * ratio * ratio * inner * wide


def score_block(left, right):
    return SCALE * jnp.einsum("id,jd->ij", left, right, preferred_element_type=jnp.float32)


def transpose_product(weights, left):
    return SCALE * jnp.einsum("ij,id->jd", weights, left, preferred_element_type=jnp.float32)


def on_device_plain(queries, documents, positives):
    norm_q, wide_q, ratio_q = normalize(queries)
    norm_d, wide_d, ratio_d = normalize(documents)
    width = lax.axis_size("blk")
    far = width // 4
    offsets = [1, -1, far, -far]
    rows = norm_q.shape[0]
    received = [norm_d]
    for off in offsets:
        received.append(from_behind(norm_d, "blk", off))
    scores = [score_block(norm_q, block) for block in received]
    total = scores[0].shape[0] * 0.0 + jnp.zeros((rows,), jnp.float32)
    for block_scores in scores:
        total = total + jnp.sum(jnp.exp(block_scores), axis=-1)
    lse = jnp.log(total)
    columns = jnp.arange(rows, dtype=jnp.int32)
    hot = (columns[None, :] == positives[0][:, None]).astype(jnp.float32)
    spos = jnp.sum(scores[0] * hot, axis=-1)
    part = jnp.sum(lse - spos)
    weights = [(jnp.exp(scores[0] - lse[:, None]) - hot).astype(jnp.bfloat16)]
    for block_scores in scores[1:]:
        weights.append(jnp.exp(block_scores - lse[:, None]).astype(jnp.bfloat16))
    query_dir = jnp.zeros_like(wide_q)
    for weight, block in zip(weights, received):
        query_dir = query_dir + SCALE * jnp.dot(weight, block, preferred_element_type=jnp.float32)
    doc_dir = transpose_product(weights[0], norm_q)
    for off, weight in zip(offsets, weights[1:]):
        partial_grad = transpose_product(weight, norm_q)
        doc_dir = doc_dir + from_behind(partial_grad.astype(jnp.bfloat16), "blk", -off).astype(
            partial_grad.dtype
        )
    query_grad = pull_back(query_dir, wide_q, ratio_q)
    doc_grad = pull_back(doc_dir, wide_d, ratio_d)
    summed = lax.psum(part, ("blk", "grp"))
    loss = summed / (rows * width * lax.axis_size("grp"))
    return (query_grad, doc_grad, loss)

CORES = 2
MESH = pl.DeviceIdType.MESH
CHUNK = 16
SPLIT = 1
PARTS = 8
LAG = 2
BUDGET = 3.5
GROUPS = (10, 4, 2)
AHEAD = 2
TILE = 512
DEEP = 1024
NEAR, DIAG, RELAY, SIBLING = range(4)


def columns(n, size):
    return pl.ds(pl.multiple_of(n * size, size), size)


def wide_dot(left, right, contract):
    return lax.dot_general(left, right, ((contract[:1], contract[1:]), ((), ())), preferred_element_type=jnp.float32)


def kernel(
    n_blk, n_grp,
    queries, documents, positives,
    query_grad, doc_grad, own, coefs, loss,
    got, norm_d, norm_q, sibling_q, group_q, scores, group_scores, weights, turned, ratio_q, ratio_d, inner,
    lse_own, lse_got, lse_wide, lse_group, sums, sums_got,
    load_sem, x_send, x_recv, y_send, y_recv, r_send, r_recv, s_send, s_recv, l_send, l_recv, t_send, t_recv,
):
    rows, width = queries.shape
    per = rows // CHUNK
    copies = 2 * per * SPLIT
    part_rows = 2 * rows // PARTS
    me, grp = lax.axis_index("blk"), lax.axis_index("grp")
    core, x, y = me % 2, (me // 2) % 2, me // 4
    sibling = me + 1 - 2 * core
    near = me + 2 - 4 * x
    across = me + 4 - 8 * y
    diag = near + 4 - 8 * y
    relay = lax.rem(me + n_blk - 1 + 2 * core, n_blk)
    relay_from = lax.rem(x + core, 2)
    peers = [(sibling, grp), (near, grp), (across, grp)]
    for bit in [1 << n for n in range(n_grp.bit_length() - 1)]:
        peers.append((me, grp + bit - 2 * bit * ((grp // bit) % 2)))

    def remote(source, target, send, recv, device):
        return pltpu.make_async_remote_copy(
            src_ref=source, dst_ref=target, send_sem=send, recv_sem=recv, device_id=device, device_id_type=MESH
        )

    def piece(n):
        size = width // SPLIT
        return (
            pl.ds(pl.multiple_of((n // SPLIT) * CHUNK, CHUNK), CHUNK),
            pl.ds(pl.multiple_of((n % SPLIT) * size, size), size),
        )

    def x_copy(n):
        r, c = piece(n)
        return remote(own.at[r, c], got.at[NEAR, r, c], x_send.at[n], x_recv.at[n], (near, grp))

    def y_copy(n):
        r, c = piece(n)
        return remote(got.at[NEAR, r, c], got.at[DIAG, r, c], y_send.at[n], y_recv.at[n], (across, grp))

    def r_copy(n):
        r, c = piece(n)
        return remote(got.at[relay_from, r, c], got.at[RELAY, r, c], r_send.at[n], r_recv.at[n], (sibling, grp))

    def s_copy(n):
        cut = pl.ds(n * part_rows, part_rows)
        return remote(own.at[cut], got.at[SIBLING, cut], s_send.at[n], s_recv.at[n], (sibling, grp))

    lse_peers = [near, diag, relay, sibling]

    def lse_copy(n):
        return remote(lse_own, lse_got.at[n], l_send.at[n], l_recv.at[n], (lse_peers[n], grp))

    def sum_copy(n):
        return remote(sums.at[n], sums_got.at[n], t_send.at[n], t_recv.at[n], peers[n])

    load_d = pltpu.make_async_copy(documents, own.at[pl.ds(0, rows)], load_sem.at[0])
    load_q = pltpu.make_async_copy(queries, own.at[pl.ds(rows, rows)], load_sem.at[1])
    load_d.start()
    load_q.start()
    group_scores[...] = jnp.zeros_like(group_scores)
    inner[1] = jnp.zeros((rows, 128), jnp.float32)
    barrier = pltpu.get_barrier_semaphore()
    greeted = peers + [(diag, grp), (relay, grp)]
    for device in greeted:
        pl.semaphore_signal(barrier, inc=1, device_id=device, device_id_type=MESH)
    pl.semaphore_wait(barrier, len(greeted))
    load_d.wait()
    for n in range(AHEAD):
        x_copy(n).start()
    load_q.wait()

    def normalized(raw):
        wide = raw.astype(jnp.float32)
        ratio = lax.rsqrt(jnp.sum(wide * wide, axis=-1, keepdims=True) + EPSILON)
        return (wide * ratio).astype(jnp.bfloat16), ratio

    def at(start, size):
        return pl.ds(start, size)

    def normalize_own(first):
        for start in range(first, first + 32, 16):
            cut = at(start, 16)
            norm_d[cut, :], ratio_d[cut, :] = normalized(own[cut, :])
            norm_q[cut, :], ratio_q[cut, :] = normalized(own[at(rows + start, 16), :])

    def normalize_into(target, target_row, source, row, count):
        for start in range(0, count, 16):
            target[at(target_row + start, 16), :] = normalized(got[source, at(row + start, 16), :])[0]

    def score(left, left_rows, right, right_rows, target):
        def body(n, _):
            cut = columns(n, DEEP)
            term = SCALE * wide_dot(left[left_rows, cut], right[right_rows, cut], (1, 1))

            @pl.when(n == 0)
            def _():
                target[...] = term

            @pl.when(n > 0)
            def _():
                target[...] += term
            return 0

        lax.fori_loop(0, width // DEEP, body, 0)

    def loop(first, last, body):
        lax.fori_loop(first, last, lambda n, _: (body(n), 0)[1], 0)

    tiles = width // TILE

    def doc_terms(left, left_rows, depth, place, first, last, low, high):
        def body(n):
            cut = columns(n, TILE)
            term = SCALE * wide_dot(turned[:, place : place + depth], left[left_rows, cut], (1, 0))
            value = term if first else doc_grad[:, cut] + term
            doc_grad[:, cut] = value
            if last:
                inner[1] += folded(own[doc_rows, cut].astype(jnp.float32) * value)

        loop(low, high, body)

    def folded(value):
        total = value[:, :128]
        for k in range(1, TILE // 128):
            total = total + value[:, k * 128 : (k + 1) * 128]
        return total


    def spread(grad, raw_rows, ratio_ref):
        ratio = ratio_ref[...]
        factor = ratio * ratio * ratio * jnp.sum(inner[0], axis=-1, keepdims=True)

        def body(n):
            cut = columns(n, TILE)
            grad[:, cut] = ratio * grad[:, cut] - factor * own[raw_rows, cut].astype(jnp.float32)

        loop(0, tiles, body)

    soon, later, state = [], [], {"now": 0, "lse": False}
    all_rows = at(0, rows)
    doc_rows, query_rows = at(0, rows), at(rows, rows)

    def block(k):
        return pl.ds(k * rows, rows)

    def put(ready, cost, step):
        later.append((ready, cost, step))

    def in_(delay, step):
        soon.append((state["now"] + delay, step))

    def send_sibling(n):
        s_copy(n).start()

    for n in range(PARTS):
        soon.append((n * SPLIT, functools.partial(send_sibling, n)))
    for first in range(0, rows, 32):
        put(0, 0.3, functools.partial(normalize_own, first))
    put(0, 1.2, lambda: score(norm_q, all_rows, norm_d, block(0), scores.at[:, block(0)]))

    def sibling_part(n):
        s_copy(n).wait_recv()
        row = n * part_rows
        if row < rows:
            normalize_into(norm_d, rows + row, SIBLING, row, part_rows)
        else:
            normalize_into(sibling_q, row - rows, SIBLING, row, part_rows)

    for n in range(PARTS):
        put((n + 2) * SPLIT, 0.3 * part_rows / 64, functools.partial(sibling_part, n))
        if (n + 1) * 2 == PARTS:
            put(0, 1.2, lambda: score(norm_q, all_rows, norm_d, block(1), scores.at[:, block(1)]))
    put(0, 1.2, lambda: score(sibling_q, all_rows, norm_d, block(0), scores.at[:, block(5)]))

    def arrived(n):
        if n < per:
            for k in (NEAR, DIAG, RELAY):
                normalize_into(norm_d, (2 + k) * rows + n * CHUNK, k, n * CHUNK, CHUNK)
        else:
            for k in (NEAR, DIAG, RELAY):
                normalize_into(group_q, ((n - per) * 3 + k) * CHUNK, k, n * CHUNK, CHUNK)

    for k in (2, 3, 4):
        put(per * SPLIT + 2, 1.2, functools.partial(
            lambda k: score(norm_q, all_rows, norm_d, block(k), scores.at[:, block(k)]), k))

    def log_sum():
        total = jnp.zeros((rows, 1), jnp.float32)
        for k in range(5):
            total = total + jnp.sum(jnp.exp(scores[:, k * rows : (k + 1) * rows]), axis=-1, keepdims=True)
        lse_wide[3] = jnp.broadcast_to(jnp.log(total), (rows, 128))
        lse_own[...] = jnp.transpose(lse_wide[3])[:8, :]
        in_(1, send_lse)

    def send_lse():
        for k in range(4):
            lse_copy(k).start()
        in_(2 * SPLIT, take_lse)

    def take_lse():
        for k in range(4):
            lse_copy(k).wait_recv()
            value = jnp.transpose(jnp.broadcast_to(lse_got[k, :1, :], (128, rows)))
            if k == SIBLING:
                lse_group[pl.ds(0, rows), :] = value
                continue
            for n in range(per):
                lse_group[pl.ds(rows + (n * 3 + k) * CHUNK, CHUNK), :] = value[n * CHUNK : (n + 1) * CHUNK, :]
        state["lse"] = True
        urgent.append((0, 0.3, sibling_weights))
        add_doc_steps(norm_q, all_rows, rows, 0, True)
        add_doc_steps(sibling_q, all_rows, rows, rows, False)

    def add_doc_steps(left, left_rows, depth, place, first, last=False):
        steps = 2 if SPLIT == 1 else 4
        for n in range(steps):
            urgent.append((0, 2.0 / steps, functools.partial(
                doc_terms, left, left_rows, depth, place, first, last, n * tiles // steps, (n + 1) * tiles // steps)))

    def sibling_weights():
        value = jnp.exp(scores[:, 5 * rows :] - lse_group[pl.ds(0, rows), :][:, :1])
        turned[:, rows : 2 * rows] = jnp.transpose(value).astype(jnp.bfloat16)

    def weight(k):
        value = jnp.exp(scores[:, k * rows : (k + 1) * rows] - lse_wide[3][:, :1])
        if k == 0:
            named = jnp.broadcast_to(positives[...].astype(jnp.float32), (rows, rows))
            place = lax.broadcasted_iota(jnp.int32, (rows, rows), 0).astype(jnp.float32)
            hot = jnp.transpose((place == named).astype(jnp.float32))
            value = value - hot
            turned[:, :rows] = jnp.transpose(value).astype(jnp.bfloat16)
            part = jnp.sum(lse_wide[3][:, :1]) - jnp.sum(scores[:, :rows] * hot)
            sums[0] = jnp.full((8, 128), part, jnp.float32)
            in_(1, functools.partial(send_sum, 0))
        weights[:, k * rows : (k + 1) * rows] = value.astype(jnp.bfloat16)

    def send_sum(n):
        sum_copy(n).start()
        in_(SPLIT, functools.partial(take_sum, n))

    def take_sum(n):
        sum_copy(n).wait_recv()
        sums[n + 1] = sums[n] + sums_got[n]
        if n + 1 < len(peers):
            in_(1, functools.partial(send_sum, n + 1))
        else:
            in_(1, give_loss)

    def give_loss():
        loss[0, 0] = jnp.max(sums[len(peers)]) / (rows * n_blk * n_grp)

    put(0, 1.0, log_sum)
    for k in range(5):
        put(0, 0.4 if k else 0.7, functools.partial(weight, k))

    def query_terms(low, high):
        def body(n):
            cut = columns(n, TILE)
            value = SCALE * wide_dot(weights[...], norm_d[:, cut], (1, 0))
            query_grad[:, cut] = value
            inner[0] += folded(own[query_rows, cut].astype(jnp.float32) * value)

        if low == 0:
            inner[0] = jnp.zeros((rows, 128), jnp.float32)
        loop(low, high, body)

    for n in range(0, tiles, 2):
        put(0, 1.0, functools.partial(query_terms, n, n + 2))
    put(0, 0.9, lambda: spread(query_grad, query_rows, ratio_q))
    urgent = []
    groups, start = [], 0
    for count in GROUPS:
        groups.append((start, count * per // 16))
        start += count * per // 16

    def group(index):
        start, count = groups[index]
        first, depth = start * 3 * CHUNK, count * 3 * CHUNK
        for low in range(0, depth, rows):
            size = min(rows, depth - low)
            urgent.append((0, 1.2, functools.partial(
                score, group_q, at(first + low, size), norm_d, block(0), group_scores.at[at(low, size), :])))

        def group_weights():
            value = jnp.exp(group_scores[at(0, depth), :] - lse_group[pl.ds(rows + first, depth), :][:, :1])
            group_scores[at(0, depth), :] = value
            turned[...] = jnp.transpose(group_scores[...]).astype(jnp.bfloat16)

        urgent.append((0, 0.5, group_weights))
        add_doc_steps(group_q, at(first, depth), depth, 0, False, index == len(groups) - 1)

    waiting = [(per + start + count - 1, n) for n, (start, count) in enumerate(groups)]
    for n in range(copies + LAG + 1):
        state["now"] = n
        if n < copies:
            x_copy(n).wait_recv()
            y_copy(n).start()
            if n + AHEAD < copies:
                x_copy(n + AHEAD).start()
        m = n - LAG
        if 0 <= m < copies:
            y_copy(m).wait_recv()
            r_copy(m).start()
        m -= 1
        if 0 <= m < copies:
            r_copy(m).wait_recv()
        ready = [step for when, step in soon if when <= n]
        soon[:] = [(when, step) for when, step in soon if when > n]
        for step in ready:
            step()
        if m >= 0 and m % SPLIT == SPLIT - 1 and m < copies:
            arrived(m // SPLIT)
        while waiting and state["lse"] and waiting[0][0] * SPLIT + SPLIT - 1 <= m:
            group(waiting.pop(0)[1])
        spent = 0.0
        while urgent or (later and later[0][0] <= n):
            pool = urgent if urgent else later
            if spent and spent + pool[0][1] > BUDGET / SPLIT:
                break
            ready, cost, step = pool.pop(0)
            step()
            spent += cost
    while soon or urgent or later or waiting:
        state["now"] += 1
        while soon:
            soon.pop(0)[1]()
        while urgent:
            urgent.pop(0)[2]()
        if later:
            later.pop(0)[2]()
        elif waiting and state["lse"]:
            group(waiting.pop(0)[1])
    ratio = ratio_d[...]
    coefs[0] = jnp.broadcast_to(ratio, (rows, 128))
    coefs[1] = jnp.broadcast_to(
        ratio * ratio * ratio * jnp.sum(inner[1], axis=-1, keepdims=True), (rows, 128)
    )

    def drain(n, _):
        x_copy(n).wait_send()
        y_copy(n).wait_send()
        r_copy(n).wait_send()
        return 0

    lax.fori_loop(0, copies, drain, 0)
    for n in range(PARTS):
        s_copy(n).wait_send()
    for k in range(4):
        lse_copy(k).wait_send()
    for k in range(len(peers)):
        sum_copy(k).wait_send()


def finish(query_grad, doc_dir, own, coefs, query_out, doc_out, staged, sem):
    rows = query_grad.shape[0]
    step = rows // 8
    copies = [pltpu.make_async_copy(query_grad, query_out, sem.at[8])]
    copies[0].start()
    for n in range(8):
        cut = pl.ds(n * step, step)
        ratio, factor = coefs[0, cut, :][:, :1], coefs[1, cut, :][:, :1]
        staged[cut, :] = ratio * doc_dir[cut, :] - factor * own[cut, :].astype(jnp.float32)
        copies.append(pltpu.make_async_copy(staged.at[cut], doc_out.at[cut], sem.at[n]))
        copies[-1].start()
    for copy in copies:
        copy.wait()


def on_device_relay(queries, documents, positives):
    n_blk, n_grp = lax.axis_size("blk"), lax.axis_size("grp")
    rows, width = queries.shape
    copies = 2 * rows // CHUNK * SPLIT
    rounds = 3 + n_grp.bit_length() - 1
    narrow, wide = jnp.bfloat16, jnp.float32
    dma = pltpu.SemaphoreType.DMA
    grad = pltpu.VMEM((rows, width), wide)
    vmem = pl.BlockSpec(memory_space=pltpu.VMEM)
    anywhere = pl.BlockSpec(memory_space=pl.ANY)
    query_grad, doc_dir, own, coefs, loss = pl.pallas_call(
        functools.partial(kernel, n_blk, n_grp),
        out_shape=[
            grad,
            grad,
            pltpu.VMEM((2 * rows, width), narrow),
            pltpu.VMEM((2, rows, 128), wide),
            jax.ShapeDtypeStruct((1, 1), wide),
        ],
        in_specs=[anywhere, anywhere, vmem],
        out_specs=[vmem, vmem, vmem, vmem, pl.BlockSpec(memory_space=pltpu.SMEM)],
        scratch_shapes=[
            pltpu.VMEM((4, 2 * rows, width), narrow),
            pltpu.VMEM((5 * rows, width), narrow),
            pltpu.VMEM((rows, width), narrow),
            pltpu.VMEM((rows, width), narrow),
            pltpu.VMEM((3 * rows, width), narrow),
            pltpu.VMEM((rows, 6 * rows), wide),
            pltpu.VMEM((2 * rows, rows), wide),
            pltpu.VMEM((rows, 5 * rows), narrow),
            pltpu.VMEM((rows, 2 * rows), narrow),
            pltpu.VMEM((rows, 1), wide),
            pltpu.VMEM((rows, 1), wide),
            pltpu.VMEM((2, rows, 128), wide),
            pltpu.VMEM((8, rows), wide),
            pltpu.VMEM((4, 8, rows), wide),
            pltpu.VMEM((4, rows, 128), wide),
            pltpu.VMEM((4 * rows, 128), wide),
            pltpu.VMEM((rounds + 1, 8, 128), wide),
            pltpu.VMEM((rounds, 8, 128), wide),
            dma((2,)),
            dma((copies,)), dma((copies,)), dma((copies,)), dma((copies,)), dma((copies,)), dma((copies,)),
            dma((PARTS,)), dma((PARTS,)), dma((4,)), dma((4,)), dma((rounds,)), dma((rounds,)),
        ],
        compiler_params=pltpu.CompilerParams(
            collective_id=0, has_side_effects=True, vmem_limit_bytes=50 * 1024 * 1024
        ),
    )(queries, documents, positives)
    out = jax.ShapeDtypeStruct((rows, width), wide)
    query_grad, doc_grad = pl.pallas_call(
        finish,
        out_shape=[out, out],
        in_specs=[vmem] * 4,
        out_specs=[anywhere, anywhere],
        scratch_shapes=[pltpu.VMEM((rows, width), wide), dma((9,))],
        compiler_params=pltpu.CompilerParams(vmem_limit_bytes=16 * 1024 * 1024),
    )(query_grad, doc_dir, own, coefs)
    return query_grad, doc_grad, loss.reshape(())


def fits(n_blk, n_grp):
    return n_blk == 4 * CORES and n_grp & (n_grp - 1) == 0


def on_device(queries, documents, positives):
    if fits(lax.axis_size("blk"), lax.axis_size("grp")):
        return on_device_relay(queries, documents, positives)
    return on_device_plain(queries, documents, positives)


def solution(mesh):
    return jax.shard_map(
        on_device,
        mesh=mesh,
        in_specs=(P(("blk", "grp"), None), P(("blk", "grp"), None), P(("blk", "grp"), None)),
        out_specs=(P(("blk", "grp"), None), P(("blk", "grp"), None), P()),
        check_vma=False,
    )
```

```python
import functools

import jax
import jax.numpy as jnp
from jax import lax
from jax.experimental import pallas as pl
from jax.experimental.pallas import tpu as pltpu
from jax.sharding import PartitionSpec as P

SCALE = 50.0
EPSILON = 1e-06


def from_behind(value, axis, steps):
    count = lax.axis_size(axis)
    pairs = [(source, (source + steps) % count) for source in range(count)]
    return lax.ppermute(value, axis, pairs)


def normalize(raw):
    wide = raw.astype(jnp.float32)
    ratio = lax.rsqrt(jnp.sum(wide * wide, axis=-1, keepdims=True) + EPSILON)
    return ((wide * ratio).astype(jnp.bfloat16), wide, ratio)


def pull_back(grad, wide, ratio):
    inner = jnp.sum(wide * grad, axis=-1, keepdims=True)
    return ratio * grad - ratio * ratio * ratio * inner * wide


def score_block(left, right):
    return SCALE * jnp.einsum("id,jd->ij", left, right, preferred_element_type=jnp.float32)


def transpose_product(weights, left):
    return SCALE * jnp.einsum("ij,id->jd", weights, left, preferred_element_type=jnp.float32)


def on_device_plain(queries, documents, positives):
    norm_q, wide_q, ratio_q = normalize(queries)
    norm_d, wide_d, ratio_d = normalize(documents)
    width = lax.axis_size("blk")
    far = width // 4
    offsets = [1, -1, far, -far]
    rows = norm_q.shape[0]
    received = [norm_d]
    for off in offsets:
        received.append(from_behind(norm_d, "blk", off))
    scores = [score_block(norm_q, block) for block in received]
    total = scores[0].shape[0] * 0.0 + jnp.zeros((rows,), jnp.float32)
    for block_scores in scores:
        total = total + jnp.sum(jnp.exp(block_scores), axis=-1)
    lse = jnp.log(total)
    columns = jnp.arange(rows, dtype=jnp.int32)
    hot = (columns[None, :] == positives[0][:, None]).astype(jnp.float32)
    spos = jnp.sum(scores[0] * hot, axis=-1)
    part = jnp.sum(lse - spos)
    weights = [(jnp.exp(scores[0] - lse[:, None]) - hot).astype(jnp.bfloat16)]
    for block_scores in scores[1:]:
        weights.append(jnp.exp(block_scores - lse[:, None]).astype(jnp.bfloat16))
    query_dir = jnp.zeros_like(wide_q)
    for weight, block in zip(weights, received):
        query_dir = query_dir + SCALE * jnp.dot(weight, block, preferred_element_type=jnp.float32)
    doc_dir = transpose_product(weights[0], norm_q)
    for off, weight in zip(offsets, weights[1:]):
        partial_grad = transpose_product(weight, norm_q)
        doc_dir = doc_dir + from_behind(partial_grad.astype(jnp.bfloat16), "blk", -off).astype(
            partial_grad.dtype
        )
    query_grad = pull_back(query_dir, wide_q, ratio_q)
    doc_grad = pull_back(doc_dir, wide_d, ratio_d)
    summed = lax.psum(part, ("blk", "grp"))
    loss = summed / (rows * width * lax.axis_size("grp"))
    return (query_grad, doc_grad, loss)

CORES = 2
MESH = pl.DeviceIdType.MESH
CHUNK = 16
SPLIT = 1
PARTS = 8
LAG = 2
BUDGET = 3.5
GROUPS = (10, 4, 2)
AHEAD = 2
TILE = 1024
DEEP = 2048
NEAR, DIAG, RELAY, SIBLING = range(4)


def columns(n, size):
    return pl.ds(pl.multiple_of(n * size, size), size)


def wide_dot(left, right, contract):
    return lax.dot_general(left, right, ((contract[:1], contract[1:]), ((), ())), preferred_element_type=jnp.float32)


def kernel(
    n_blk, n_grp,
    queries, documents, positives,
    query_grad, doc_grad, own, coefs, loss,
    got, norm_d, norm_q, sibling_q, group_q, scores, group_scores, weights, turned, ratio_q, ratio_d, inner,
    lse_own, lse_got, lse_wide, lse_group, sums, sums_got,
    load_sem, x_send, x_recv, y_send, y_recv, r_send, r_recv, s_send, s_recv, l_send, l_recv, t_send, t_recv,
):
    rows, width = queries.shape
    per = rows // CHUNK
    copies = 2 * per * SPLIT
    part_rows = 2 * rows // PARTS
    me, grp = lax.axis_index("blk"), lax.axis_index("grp")
    core, x, y = me % 2, (me // 2) % 2, me // 4
    sibling = me + 1 - 2 * core
    near = me + 2 - 4 * x
    across = me + 4 - 8 * y
    diag = near + 4 - 8 * y
    relay = lax.rem(me + n_blk - 1 + 2 * core, n_blk)
    relay_from = lax.rem(x + core, 2)
    peers = [(sibling, grp), (near, grp), (across, grp)]
    for bit in [1 << n for n in range(n_grp.bit_length() - 1)]:
        peers.append((me, grp + bit - 2 * bit * ((grp // bit) % 2)))

    def remote(source, target, send, recv, device):
        return pltpu.make_async_remote_copy(
            src_ref=source, dst_ref=target, send_sem=send, recv_sem=recv, device_id=device, device_id_type=MESH
        )

    def piece(n):
        size = width // SPLIT
        return (
            pl.ds(pl.multiple_of((n // SPLIT) * CHUNK, CHUNK), CHUNK),
            pl.ds(pl.multiple_of((n % SPLIT) * size, size), size),
        )

    def x_copy(n):
        r, c = piece(n)
        return remote(own.at[r, c], got.at[NEAR, r, c], x_send.at[n], x_recv.at[n], (near, grp))

    def y_copy(n):
        r, c = piece(n)
        return remote(got.at[NEAR, r, c], got.at[DIAG, r, c], y_send.at[n], y_recv.at[n], (across, grp))

    def r_copy(n):
        r, c = piece(n)
        return remote(got.at[relay_from, r, c], got.at[RELAY, r, c], r_send.at[n], r_recv.at[n], (sibling, grp))

    def s_copy(n):
        cut = pl.ds(n * part_rows, part_rows)
        return remote(own.at[cut], got.at[SIBLING, cut], s_send.at[n], s_recv.at[n], (sibling, grp))

    lse_peers = [near, diag, relay, sibling]

    def lse_copy(n):
        return remote(lse_own, lse_got.at[n], l_send.at[n], l_recv.at[n], (lse_peers[n], grp))

    def sum_copy(n):
        return remote(sums.at[n], sums_got.at[n], t_send.at[n], t_recv.at[n], peers[n])

    load_d = pltpu.make_async_copy(documents, own.at[pl.ds(0, rows)], load_sem.at[0])
    load_q = pltpu.make_async_copy(queries, own.at[pl.ds(rows, rows)], load_sem.at[1])
    load_d.start()
    load_q.start()
    group_scores[...] = jnp.zeros_like(group_scores)
    inner[1] = jnp.zeros((rows, 128), jnp.float32)
    barrier = pltpu.get_barrier_semaphore()
    greeted = peers + [(diag, grp), (relay, grp)]
    for device in greeted:
        pl.semaphore_signal(barrier, inc=1, device_id=device, device_id_type=MESH)
    pl.semaphore_wait(barrier, len(greeted))
    load_d.wait()
    for n in range(AHEAD):
        x_copy(n).start()
    load_q.wait()

    def normalized(raw):
        wide = raw.astype(jnp.float32)
        ratio = lax.rsqrt(jnp.sum(wide * wide, axis=-1, keepdims=True) + EPSILON)
        return (wide * ratio).astype(jnp.bfloat16), ratio

    def at(start, size):
        return pl.ds(start, size)

    def normalize_own(first):
        for start in range(first, first + 32, 16):
            cut = at(start, 16)
            norm_d[cut, :], ratio_d[cut, :] = normalized(own[cut, :])
            norm_q[cut, :], ratio_q[cut, :] = normalized(own[at(rows + start, 16), :])

    def normalize_into(target, target_row, source, row, count):
        for start in range(0, count, 16):
            target[at(target_row + start, 16), :] = normalized(got[source, at(row + start, 16), :])[0]

    def score(left, left_rows, right, right_rows, target):
        def body(n, _):
            cut = columns(n, DEEP)
            term = SCALE * wide_dot(left[left_rows, cut], right[right_rows, cut], (1, 1))

            @pl.when(n == 0)
            def _():
                target[...] = term

            @pl.when(n > 0)
            def _():
                target[...] += term
            return 0

        lax.fori_loop(0, width // DEEP, body, 0)

    def loop(first, last, body):
        lax.fori_loop(first, last, lambda n, _: (body(n), 0)[1], 0)

    tiles = width // TILE

    def doc_terms(left, left_rows, depth, place, first, last, low, high):
        def body(n):
            cut = columns(n, TILE)
            term = SCALE * wide_dot(turned[:, place : place + depth], left[left_rows, cut], (1, 0))
            value = term if first else doc_grad[:, cut] + term
            doc_grad[:, cut] = value
            if last:
                inner[1] += folded(own[doc_rows, cut].astype(jnp.float32) * value)

        loop(low, high, body)

    def folded(value):
        total = value[:, :128]
        for k in range(1, TILE // 128):
            total = total + value[:, k * 128 : (k + 1) * 128]
        return total


    def spread(grad, raw_rows, ratio_ref):
        ratio = ratio_ref[...]
        factor = ratio * ratio * ratio * jnp.sum(inner[0], axis=-1, keepdims=True)

        def body(n):
            cut = columns(n, TILE)
            grad[:, cut] = ratio * grad[:, cut] - factor * own[raw_rows, cut].astype(jnp.float32)

        loop(0, tiles, body)

    soon, later, state = [], [], {"now": 0, "lse": False}
    all_rows = at(0, rows)
    doc_rows, query_rows = at(0, rows), at(rows, rows)

    def block(k):
        return pl.ds(k * rows, rows)

    def put(ready, cost, step):
        later.append((ready, cost, step))

    def in_(delay, step):
        soon.append((state["now"] + delay, step))

    def send_sibling(n):
        s_copy(n).start()

    for n in range(PARTS):
        soon.append((n * SPLIT, functools.partial(send_sibling, n)))
    for first in range(0, rows, 32):
        put(0, 0.3, functools.partial(normalize_own, first))
    put(0, 1.2, lambda: score(norm_q, all_rows, norm_d, block(0), scores.at[:, block(0)]))

    def sibling_part(n):
        s_copy(n).wait_recv()
        row = n * part_rows
        if row < rows:
            normalize_into(norm_d, rows + row, SIBLING, row, part_rows)
        else:
            normalize_into(sibling_q, row - rows, SIBLING, row, part_rows)

    for n in range(PARTS):
        put((n + 2) * SPLIT, 0.3 * part_rows / 64, functools.partial(sibling_part, n))
        if (n + 1) * 2 == PARTS:
            put(0, 1.2, lambda: score(norm_q, all_rows, norm_d, block(1), scores.at[:, block(1)]))
    put(0, 1.2, lambda: score(sibling_q, all_rows, norm_d, block(0), scores.at[:, block(5)]))

    def arrived(n):
        if n < per:
            for k in (NEAR, DIAG, RELAY):
                normalize_into(norm_d, (2 + k) * rows + n * CHUNK, k, n * CHUNK, CHUNK)
        else:
            for k in (NEAR, DIAG, RELAY):
                normalize_into(group_q, ((n - per) * 3 + k) * CHUNK, k, n * CHUNK, CHUNK)

    for k in (2, 3, 4):
        put(per * SPLIT + 2, 1.2, functools.partial(
            lambda k: score(norm_q, all_rows, norm_d, block(k), scores.at[:, block(k)]), k))

    def log_sum():
        total = jnp.zeros((rows, 1), jnp.float32)
        for k in range(5):
            total = total + jnp.sum(jnp.exp(scores[:, k * rows : (k + 1) * rows]), axis=-1, keepdims=True)
        lse_wide[3] = jnp.broadcast_to(jnp.log(total), (rows, 128))
        lse_own[...] = jnp.transpose(lse_wide[3])[:8, :]
        in_(1, send_lse)

    def send_lse():
        for k in range(4):
            lse_copy(k).start()
        in_(2 * SPLIT, take_lse)

    def take_lse():
        for k in range(4):
            lse_copy(k).wait_recv()
            value = jnp.transpose(jnp.broadcast_to(lse_got[k, :1, :], (128, rows)))
            if k == SIBLING:
                lse_group[pl.ds(0, rows), :] = value
                continue
            for n in range(per):
                lse_group[pl.ds(rows + (n * 3 + k) * CHUNK, CHUNK), :] = value[n * CHUNK : (n + 1) * CHUNK, :]
        state["lse"] = True
        urgent.append((0, 0.3, sibling_weights))
        add_doc_steps(norm_q, all_rows, rows, 0, True)
        add_doc_steps(sibling_q, all_rows, rows, rows, False)

    def add_doc_steps(left, left_rows, depth, place, first, last=False):
        steps = 2 if SPLIT == 1 else 4
        for n in range(steps):
            urgent.append((0, 2.0 / steps, functools.partial(
                doc_terms, left, left_rows, depth, place, first, last, n * tiles // steps, (n + 1) * tiles // steps)))

    def sibling_weights():
        value = jnp.exp(scores[:, 5 * rows :] - lse_group[pl.ds(0, rows), :][:, :1])
        turned[:, rows : 2 * rows] = jnp.transpose(value).astype(jnp.bfloat16)

    def weight(k):
        value = jnp.exp(scores[:, k * rows : (k + 1) * rows] - lse_wide[3][:, :1])
        if k == 0:
            named = jnp.broadcast_to(positives[...].astype(jnp.float32), (rows, rows))
            place = lax.broadcasted_iota(jnp.int32, (rows, rows), 0).astype(jnp.float32)
            hot = jnp.transpose((place == named).astype(jnp.float32))
            value = value - hot
            turned[:, :rows] = jnp.transpose(value).astype(jnp.bfloat16)
            part = jnp.sum(lse_wide[3][:, :1]) - jnp.sum(scores[:, :rows] * hot)
            sums[0] = jnp.full((8, 128), part, jnp.float32)
            in_(1, functools.partial(send_sum, 0))
        weights[:, k * rows : (k + 1) * rows] = value.astype(jnp.bfloat16)

    def send_sum(n):
        sum_copy(n).start()
        in_(SPLIT, functools.partial(take_sum, n))

    def take_sum(n):
        sum_copy(n).wait_recv()
        sums[n + 1] = sums[n] + sums_got[n]
        if n + 1 < len(peers):
            in_(1, functools.partial(send_sum, n + 1))
        else:
            in_(1, give_loss)

    def give_loss():
        loss[0, 0] = jnp.max(sums[len(peers)]) / (rows * n_blk * n_grp)

    put(0, 1.0, log_sum)
    for k in range(5):
        put(0, 0.4 if k else 0.7, functools.partial(weight, k))

    def query_terms(low, high):
        def body(n):
            cut = columns(n, TILE)
            value = SCALE * wide_dot(weights[...], norm_d[:, cut], (1, 0))
            query_grad[:, cut] = value
            inner[0] += folded(own[query_rows, cut].astype(jnp.float32) * value)

        if low == 0:
            inner[0] = jnp.zeros((rows, 128), jnp.float32)
        loop(low, high, body)

    for n in range(0, tiles, 2):
        put(0, 1.0, functools.partial(query_terms, n, n + 2))
    put(0, 0.9, lambda: spread(query_grad, query_rows, ratio_q))
    urgent = []
    groups, start = [], 0
    for count in GROUPS:
        groups.append((start, count * per // 16))
        start += count * per // 16

    def group(index):
        start, count = groups[index]
        first, depth = start * 3 * CHUNK, count * 3 * CHUNK
        for low in range(0, depth, rows):
            size = min(rows, depth - low)
            urgent.append((0, 1.2, functools.partial(
                score, group_q, at(first + low, size), norm_d, block(0), group_scores.at[at(low, size), :])))

        def group_weights():
            value = jnp.exp(group_scores[at(0, depth), :] - lse_group[pl.ds(rows + first, depth), :][:, :1])
            group_scores[at(0, depth), :] = value
            turned[...] = jnp.transpose(group_scores[...]).astype(jnp.bfloat16)

        urgent.append((0, 0.5, group_weights))
        add_doc_steps(group_q, at(first, depth), depth, 0, False, index == len(groups) - 1)

    waiting = [(per + start + count - 1, n) for n, (start, count) in enumerate(groups)]
    for n in range(copies + LAG + 1):
        state["now"] = n
        if n < copies:
            x_copy(n).wait_recv()
            y_copy(n).start()
            if n + AHEAD < copies:
                x_copy(n + AHEAD).start()
        m = n - LAG
        if 0 <= m < copies:
            y_copy(m).wait_recv()
            r_copy(m).start()
        m -= 1
        if 0 <= m < copies:
            r_copy(m).wait_recv()
        ready = [step for when, step in soon if when <= n]
        soon[:] = [(when, step) for when, step in soon if when > n]
        for step in ready:
            step()
        if m >= 0 and m % SPLIT == SPLIT - 1 and m < copies:
            arrived(m // SPLIT)
        while waiting and state["lse"] and waiting[0][0] * SPLIT + SPLIT - 1 <= m:
            group(waiting.pop(0)[1])
        spent = 0.0
        while urgent or (later and later[0][0] <= n):
            pool = urgent if urgent else later
            if spent and spent + pool[0][1] > BUDGET / SPLIT:
                break
            ready, cost, step = pool.pop(0)
            step()
            spent += cost
    while soon or urgent or later or waiting:
        state["now"] += 1
        while soon:
            soon.pop(0)[1]()
        while urgent:
            urgent.pop(0)[2]()
        if later:
            later.pop(0)[2]()
        elif waiting and state["lse"]:
            group(waiting.pop(0)[1])
    ratio = ratio_d[...]
    coefs[0] = jnp.broadcast_to(ratio, (rows, 128))
    coefs[1] = jnp.broadcast_to(
        ratio * ratio * ratio * jnp.sum(inner[1], axis=-1, keepdims=True), (rows, 128)
    )

    def drain(n, _):
        x_copy(n).wait_send()
        y_copy(n).wait_send()
        r_copy(n).wait_send()
        return 0

    lax.fori_loop(0, copies, drain, 0)
    for n in range(PARTS):
        s_copy(n).wait_send()
    for k in range(4):
        lse_copy(k).wait_send()
    for k in range(len(peers)):
        sum_copy(k).wait_send()


def finish(query_grad, doc_dir, own, coefs, query_out, doc_out, staged, sem):
    rows = query_grad.shape[0]
    step = rows // 8
    copies = [pltpu.make_async_copy(query_grad, query_out, sem.at[8])]
    copies[0].start()
    for n in range(8):
        cut = pl.ds(n * step, step)
        ratio, factor = coefs[0, cut, :][:, :1], coefs[1, cut, :][:, :1]
        staged[cut, :] = ratio * doc_dir[cut, :] - factor * own[cut, :].astype(jnp.float32)
        copies.append(pltpu.make_async_copy(staged.at[cut], doc_out.at[cut], sem.at[n]))
        copies[-1].start()
    for copy in copies:
        copy.wait()


def on_device_relay(queries, documents, positives):
    n_blk, n_grp = lax.axis_size("blk"), lax.axis_size("grp")
    rows, width = queries.shape
    copies = 2 * rows // CHUNK * SPLIT
    rounds = 3 + n_grp.bit_length() - 1
    narrow, wide = jnp.bfloat16, jnp.float32
    dma = pltpu.SemaphoreType.DMA
    grad = pltpu.VMEM((rows, width), wide)
    vmem = pl.BlockSpec(memory_space=pltpu.VMEM)
    anywhere = pl.BlockSpec(memory_space=pl.ANY)
    query_grad, doc_dir, own, coefs, loss = pl.pallas_call(
        functools.partial(kernel, n_blk, n_grp),
        out_shape=[
            grad,
            grad,
            pltpu.VMEM((2 * rows, width), narrow),
            pltpu.VMEM((2, rows, 128), wide),
            jax.ShapeDtypeStruct((1, 1), wide),
        ],
        in_specs=[anywhere, anywhere, vmem],
        out_specs=[vmem, vmem, vmem, vmem, pl.BlockSpec(memory_space=pltpu.SMEM)],
        scratch_shapes=[
            pltpu.VMEM((4, 2 * rows, width), narrow),
            pltpu.VMEM((5 * rows, width), narrow),
            pltpu.VMEM((rows, width), narrow),
            pltpu.VMEM((rows, width), narrow),
            pltpu.VMEM((3 * rows, width), narrow),
            pltpu.VMEM((rows, 6 * rows), wide),
            pltpu.VMEM((2 * rows, rows), wide),
            pltpu.VMEM((rows, 5 * rows), narrow),
            pltpu.VMEM((rows, 2 * rows), narrow),
            pltpu.VMEM((rows, 1), wide),
            pltpu.VMEM((rows, 1), wide),
            pltpu.VMEM((2, rows, 128), wide),
            pltpu.VMEM((8, rows), wide),
            pltpu.VMEM((4, 8, rows), wide),
            pltpu.VMEM((4, rows, 128), wide),
            pltpu.VMEM((4 * rows, 128), wide),
            pltpu.VMEM((rounds + 1, 8, 128), wide),
            pltpu.VMEM((rounds, 8, 128), wide),
            dma((2,)),
            dma((copies,)), dma((copies,)), dma((copies,)), dma((copies,)), dma((copies,)), dma((copies,)),
            dma((PARTS,)), dma((PARTS,)), dma((4,)), dma((4,)), dma((rounds,)), dma((rounds,)),
        ],
        compiler_params=pltpu.CompilerParams(
            collective_id=0, has_side_effects=True, vmem_limit_bytes=50 * 1024 * 1024
        ),
    )(queries, documents, positives)
    out = jax.ShapeDtypeStruct((rows, width), wide)
    query_grad, doc_grad = pl.pallas_call(
        finish,
        out_shape=[out, out],
        in_specs=[vmem] * 4,
        out_specs=[anywhere, anywhere],
        scratch_shapes=[pltpu.VMEM((rows, width), wide), dma((9,))],
        compiler_params=pltpu.CompilerParams(vmem_limit_bytes=16 * 1024 * 1024),
    )(query_grad, doc_dir, own, coefs)
    return query_grad, doc_grad, loss.reshape(())


def fits(n_blk, n_grp):
    return n_blk == 4 * CORES and n_grp & (n_grp - 1) == 0


def on_device(queries, documents, positives):
    if fits(lax.axis_size("blk"), lax.axis_size("grp")):
        return on_device_relay(queries, documents, positives)
    return on_device_plain(queries, documents, positives)


def solution(mesh):
    return jax.shard_map(
        on_device,
        mesh=mesh,
        in_specs=(P(("blk", "grp"), None), P(("blk", "grp"), None), P(("blk", "grp"), None)),
        out_specs=(P(("blk", "grp"), None), P(("blk", "grp"), None), P()),
        check_vma=False,
    )
```
